32 devices in a mesh: ctx: 16 (over z, x, core), tp: 2 (over y).
Axes of the slice: x: 2, y: 2, z: 4, core: 2. Of those that a mesh axis runs over, the one named last changes fastest.
Arguments:
- token_ids: int32 [12288], P('ctx'), may hold values from 0 to 511
- embed_table: bfloat16 [512, 4096], replicated, may hold values from -6 to 6
- norm_gain: float32 [4096], replicated, may hold values from 0.25 to 1.75
- w_in: bfloat16 [4096, 3, 2048], P(None, None, 'tp'), may hold values from -0.09375 to 0.09375
- short_taps: float32 [3, 3, 2048], P(None, None, 'tp'), may hold values from -3 to 3
- long_filter: bfloat16 [2048, 12288], P('tp', 'ctx'), may hold values from -0.0546875 to 0.0546875
- skip_gain: float32 [2048], P('tp'), may hold values from 0.5 to 2
- w_out: bfloat16 [2048, 4096], P(None, 'tp'), may hold values from -0.125 to 0.125
Outputs:
- mixed: bfloat16 [12288, 4096], P('ctx', 'tp')
The draws below stay inside these ranges and needn't reach their ends.
All inputs are finite; a program needn't handle non-finite values.
Results may differ from the reference program's by a relative error of at most 0.0095.
Values may be sent and summed in bfloat16 or wider, within the bound.
A program may use at most 192 MiB of HBM per device.

```python
import math
import jax
import jax.numpy as jnp
import numpy as np
from jax import lax

D = 4096
C = 2048
V = 512
SEQ = 12288


def touch_ends(result, stream_key, smallest, largest):
    longest = result.shape.index(max(result.shape))
    spots = []
    for shift in (0, 1):
        where = [jax.random.randint(jax.random.fold_in(stream_key, axis), (), 0, length) for axis, length in enumerate(result.shape)]
        where[longest] = (where[longest] + shift) % result.shape[longest]
        spots.append(tuple(where))
    return result.at[spots[0]].set(smallest).at[spots[1]].set(largest)


def block_levels(stream_key, extent, split, least, largest):
    def one(axis_at, parts):
        draws = jax.random.uniform(jax.random.fold_in(jax.random.fold_in(stream_key, 6), axis_at), (parts,), jnp.float32, least / len(split), largest / len(split))
        return jnp.repeat(jnp.exp(draws), extent[axis_at] // parts).reshape((-1,) + (1,) * (len(extent) - axis_at - 1))

    factor_of = one(*split[0])
    for cut in split[1:]:
        factor_of = factor_of * one(*cut)
    return factor_of


def rank_bounds(amount, lean):
    weights = [(1 << 20) // math.isqrt(grade ** lean) + 1 for grade in range(1, amount + 1)]
    deviation = 1 + sum(weights) // (1 << 30)
    return np.cumsum(np.array([max(1, weight // deviation) for weight in weights]))


def skewed_ids(rng, shape, amount, lean):
    listing = rank_bounds(amount, lean)
    ticket = jax.random.randint(jax.random.fold_in(rng, 1), shape, 0, int(listing[amount - 1]))
    grade = jnp.searchsorted(jnp.asarray(listing, jnp.int32), ticket, side="right")
    return jax.random.permutation(jax.random.fold_in(rng, 2), amount)[grade].astype(jnp.int32)


def scatter_about(rng, dims, deviation, limit, cuts=(), dtype=jnp.bfloat16):
    drawn = deviation * jax.random.normal(rng, dims, jnp.float32)
    if cuts:
        drawn = drawn * block_levels(rng, dims, cuts, -0.22, 0.18)
    return jnp.clip(drawn, -limit, limit).astype(dtype)


def setup_inputs(seed: int = 0) -> dict:
    seeds = jax.random.split(jax.random.key(seed), 9)
    return {
        "token_ids": touch_ends(skewed_ids(seeds[0], (SEQ,), V, 2), jax.random.fold_in(seeds[0], 3), 0, V - 1).astype(jnp.int32),
        "embed_table": scatter_about(seeds[1], (V, D), 1.0, 6.0),
        "norm_gain": jnp.clip(1.0 + 0.15 * jax.random.normal(seeds[2], (D,), jnp.float32), 0.25, 1.75),
        "w_in": scatter_about(seeds[3], (D, 3, C), D ** -0.5, 0.09375, ((2, 2),)),
        "short_taps": scatter_about(seeds[4], (3, 3, C), 0.6, 3.0, ((2, 2),), jnp.float32),
        "long_filter": scatter_about(seeds[5], (C, SEQ), SEQ ** -0.5, 0.0546875, ((0, 2), (1, 16))),
        "skip_gain": jnp.clip(0.5 + 1.5 * jax.random.uniform(seeds[6], (C,), jnp.float32) ** block_levels(seeds[6], (C,), ((0, 2),), -0.2, 0.2), 0.5, 2.0),
        "w_out": scatter_about(seeds[7], (C, D), C ** -0.5, 0.125, ((1, 2),)),
    }


norm_eps = 1e-06

def causal_conv(pair):
    signal, kernel = pair
    length = signal.shape[-1]
    spectrum = jnp.fft.rfft(signal, n=2 * length, axis=-1) * jnp.fft.rfft(kernel, n=2 * length, axis=-1)
    return jnp.fft.irfft(spectrum, n=2 * length, axis=-1)[:, :length]

def reference(token_ids, embed_table, norm_gain, w_in, short_taps, long_filter, skip_gain, w_out):
    embedded = jnp.take(embed_table, token_ids, axis=0).astype(jnp.float32)
    scale = lax.rsqrt(lax.optimization_barrier(jnp.mean(embedded * embedded, axis=1, keepdims=True)) + norm_eps)
    normed = (embedded * scale * norm_gain).astype(jnp.bfloat16)
    width = normed.shape[1]
    channels = w_in.shape[2]
    projected = jnp.dot(normed.astype(jnp.float32), w_in.reshape(width, 3 * channels).astype(jnp.float32), precision=lax.Precision.HIGHEST, preferred_element_type=jnp.float32)
    projected = lax.optimization_barrier(projected.astype(jnp.bfloat16))
    projected = projected.reshape(-1, 3, channels).astype(jnp.float32)
    once = jnp.pad(projected, ((1, 0), (0, 0), (0, 0)))[:-1]
    twice = jnp.pad(projected, ((2, 0), (0, 0), (0, 0)))[:-2]
    shortened = short_taps[0] * projected + short_taps[1] * once + short_taps[2] * twice
    shortened = lax.optimization_barrier(shortened.astype(jnp.bfloat16)).astype(jnp.float32)
    query = shortened[:, 0, :].T
    key_side = shortened[:, 1, :]
    value_side = shortened[:, 2, :]
    product = lax.optimization_barrier((key_side * value_side).astype(jnp.bfloat16))
    product = product.astype(jnp.float32).T
    length = product.shape[1]
    filters = long_filter.astype(jnp.float32)
    block = 128
    convolved = lax.map(causal_conv, (product.reshape(channels // block, block, length), filters.reshape(channels // block, block, length)))
    convolved = convolved.reshape(channels, length)
    skipped = lax.optimization_barrier((convolved + skip_gain[:, None] * product).astype(jnp.bfloat16))
    gated = (query * skipped.astype(jnp.float32)).astype(jnp.bfloat16)
    gated_rows = gated.astype(jnp.float32).T
    projected_out = jnp.dot(gated_rows, w_out.astype(jnp.float32), precision=lax.Precision.HIGHEST, preferred_element_type=jnp.float32)
    return (embedded + projected_out).astype(jnp.bfloat16)
```

```python
import functools
import math

import jax
import jax.numpy as jnp
import numpy as np
from jax import lax
from jax.experimental import pallas as pl
from jax.experimental.pallas import tpu as pltpu
from jax.sharding import PartitionSpec as P

norm_eps = 1e-06
lanes = 128
wide = 256


def transform_tables(length):
    period = 2 * length
    rows = length // lanes
    kept = rows + 1
    padded = -(-kept // 16) * 16
    coarse = np.zeros((2 * padded, rows))
    grid = 2 * np.pi * (np.outer(np.arange(kept), np.arange(rows)) % (2 * rows)) / (2 * rows)
    coarse[:kept] = np.cos(grid)
    coarse[padded : padded + kept] = -np.sin(grid)
    weight = np.full((kept, 1), 2.0)
    weight[0] = weight[-1] = 1.0
    back = np.zeros((rows, 2 * padded))
    back[:, :kept] = (weight * np.cos(grid)).T / period
    back[:, padded : padded + kept] = -(weight * np.sin(grid)).T / period
    turn = 2 * np.pi * np.outer(np.arange(padded), np.arange(lanes)) / period
    fine = 2 * np.pi * (np.outer(np.arange(lanes), np.arange(lanes)) % lanes) / lanes
    cos, sin = np.cos(fine), np.sin(fine)
    forward = np.block([[cos, -sin], [sin, cos]])
    inverse = np.block([[cos, sin], [-sin, cos]])
    half = jnp.bfloat16
    return (
        coarse.astype(half),
        np.cos(turn).astype(np.float32),
        np.sin(turn).astype(np.float32),
        forward.astype(half),
        inverse.astype(half),
        back.astype(half),
    )


def mul(left, right):
    return jnp.dot(left, right, preferred_element_type=jnp.float32)


def block_kernel(
    tok_ref, tab_ref, taps_ref, skip_ref, h_ref,
    coarse_ref, cos_ref, sin_ref, fwd_ref, inv_ref, back_ref,
    out_ref, pf, hf, q_s, p_s, *, stride, unroll,
):
    half = jnp.bfloat16
    full = jnp.float32
    sources, chans, span = h_ref.shape
    per = span // lanes
    blocks = sources * per
    vocab = tab_ref.shape[1]
    rows3 = 3 * chans
    padded = cos_ref.shape[0]

    words = lax.broadcasted_iota(jnp.int32, (vocab, wide), 0)
    lane = lax.broadcasted_iota(jnp.int32, (rows3, lanes), 1)

    def project(step, carry):
        one_back, two_back = carry
        picked = jnp.where(words == tok_ref[pl.ds(step, 1), :], 1.0, 0.0).astype(half)
        both = mul(tab_ref[...], picked).astype(half).astype(full)
        for part in range(wide // lanes):
            now = both[:, part * lanes : (part + 1) * lanes]
            once = pltpu.roll(now, 1, 1)
            twice = pltpu.roll(now, 2, 1)
            short = (
                taps_ref[0] * now
                + taps_ref[1] * jnp.where(lane < 1, one_back, once)
                + taps_ref[2] * jnp.where(lane < 2, two_back, twice)
            ).astype(half)
            one_back, two_back = once, twice
            key = short[chans : 2 * chans].astype(full)
            value = short[2 * chans :].astype(full)
            product = (key * value).astype(half)
            at = step * (wide // lanes) + part
            q_s[at] = short[:chans]
            p_s[at] = product
            pf[pl.ds(at, chans, stride=stride), :] = product.astype(full)
        return one_back, two_back

    zero = jnp.zeros((rows3, lanes), full)
    lax.fori_loop(0, blocks * lanes // wide, project, (zero, zero))

    def take(source, _):
        for part in range(per):
            tile = h_ref[source, :, part * lanes : (part + 1) * lanes]
            hf[pl.ds(source * per + part, chans, stride=stride), :] = tile.astype(full)
        return 0

    lax.fori_loop(0, sources, take, 0)

    def convolve(step, _):
        for sub in range(unroll):
            first = pl.multiple_of((step * unroll + sub) * stride, 8)
            here = pl.ds(first, blocks)
            pair = jnp.concatenate([pf[here, :].astype(half), hf[here, :].astype(half)], axis=1)
            staged = mul(coarse_ref[...], pair)
            cos, sin = cos_ref[...], sin_ref[...]

            def turned(lo):
                real = staged[:padded, lo : lo + lanes]
                imag = staged[padded:, lo : lo + lanes]
                return jnp.concatenate(
                    [(real * cos + imag * sin).astype(half), (imag * cos - real * sin).astype(half)],
                    axis=1,
                )

            spectra = mul(jnp.concatenate([turned(0), turned(lanes)], axis=0), fwd_ref[...])
            pr, pi = spectra[:padded, :lanes], spectra[:padded, lanes:]
            hr, hi = spectra[padded:, :lanes], spectra[padded:, lanes:]
            joint = jnp.concatenate(
                [(pr * hr - pi * hi).astype(half), (pr * hi + pi * hr).astype(half)], axis=1
            )
            undone = mul(joint, inv_ref[...])
            br, bi = undone[:, :lanes], undone[:, lanes:]
            stacked = jnp.concatenate(
                [(br * cos - bi * sin).astype(half), (bi * cos + br * sin).astype(half)], axis=0
            )
            pf[here, :] = mul(back_ref[...], stacked)
        return 0

    lax.fori_loop(0, chans // unroll, convolve, 0)

    def finish(source, _):
        for part in range(per):
            at = source * per + part
            convolved = pf[pl.ds(at, chans, stride=stride), :]
            skipped = (convolved + skip_ref[...] * p_s[at].astype(full)).astype(half)
            gated = q_s[at].astype(full) * skipped.astype(full)
            out_ref[source, :, part * lanes : (part + 1) * lanes] = gated.astype(half)
        return 0

    lax.fori_loop(0, sources, finish, 0)


def long_block(tokens, table, taps, skip, filters, chans):
    groups, _, span = filters.shape
    length = groups * span
    blocks = length // lanes
    stride = blocks + 8
    tables = transform_tables(length)
    unroll = math.gcd(chans, 4)
    vmem = pl.BlockSpec(memory_space=pltpu.VMEM)
    return pl.pallas_call(
        functools.partial(block_kernel, stride=stride, unroll=unroll),
        out_shape=jax.ShapeDtypeStruct((groups, chans, span), jnp.bfloat16),
        in_specs=[vmem] * 11,
        out_specs=vmem,
        scratch_shapes=[
            pltpu.VMEM((chans * stride, lanes), jnp.float32),
            pltpu.VMEM((chans * stride, lanes), jnp.float32),
            pltpu.VMEM((blocks, chans, lanes), jnp.bfloat16),
            pltpu.VMEM((blocks, chans, lanes), jnp.bfloat16),
        ],
        compiler_params=pltpu.CompilerParams(vmem_limit_bytes=48 * 1024 * 1024),
        cost_estimate=pl.CostEstimate(
            flops=40_000_000_000, bytes_accessed=8_000_000, transcendentals=0
        ),
    )(tokens.reshape(length // wide, wide), table, taps, skip, filters, *map(jnp.asarray, tables))


def local(token_ids, embed_table, norm_gain, w_in, short_taps, long_filter, skip_gain, w_out):
    half = jnp.bfloat16
    vocab, width = embed_table.shape
    local_channels = w_in.shape[2]
    groups = lax.axis_size("ctx")
    parts = lax.axis_size("tp")
    me = lax.axis_index("tp")
    chans = local_channels // groups
    first = lax.axis_index("ctx") * chans
    span = token_ids.shape[0]

    filters = lax.all_to_all(
        long_filter.reshape(groups, chans, span), "ctx", split_axis=0, concat_axis=0, tiled=True
    )
    tokens = lax.all_gather(token_ids, "ctx", axis=0, tiled=True)

    rows = embed_table.astype(jnp.float32)
    scale = lax.rsqrt(jnp.mean(rows * rows, axis=1, keepdims=True) + norm_eps)
    normed = (rows * scale * norm_gain).astype(half)
    own_w = lax.dynamic_slice_in_dim(w_in, first, chans, 2).reshape(width, 3 * chans)
    table = lax.dot_general(
        own_w, normed, (((0,), (1,)), ((), ())), preferred_element_type=jnp.float32
    ).astype(half)
    taps = lax.dynamic_slice_in_dim(short_taps, first, chans, 2).reshape(-1, 3 * chans, 1)
    skip = lax.dynamic_slice_in_dim(skip_gain, first, chans)[:, None]

    gated = long_block(tokens, table, taps, skip, filters, chans)
    mine = lax.all_to_all(gated, "ctx", split_axis=0, concat_axis=0, tiled=True)
    mine = mine.reshape(local_channels, span)

    columns = w_out.shape[1]
    one_hot = (token_ids[:, None] == jnp.arange(vocab, dtype=jnp.int32)[None, :]).astype(half)
    own_embed = lax.dynamic_slice_in_dim(embed_table, me * columns, columns, 1)
    total = jnp.dot(one_hot, own_embed, preferred_element_type=jnp.float32)
    for step in range(parts):
        if step == 0:
            piece = mine
        else:
            route = [(i, (i + step) % parts) for i in range(parts)]
            piece = lax.ppermute(mine, "tp", route)
        owner = lax.rem(me - step + parts, parts)
        own_rows = lax.dynamic_slice_in_dim(w_out, owner * local_channels, local_channels, 0)
        total = total + lax.dot_general(
            piece, own_rows, (((0,), (0,)), ((), ())), preferred_element_type=jnp.float32
        )
    return total.astype(half)


def solution(mesh):
    return jax.shard_map(
        local,
        mesh=mesh,
        in_specs=(
            P("ctx"),
            P(),
            P(),
            P(None, None, "tp"),
            P(None, None, "tp"),
            P("tp", "ctx"),
            P("tp"),
            P(None, "tp"),
        ),
        out_specs=P("ctx", "tp"),
        check_vma=False,
    )
```

```python
import functools
import math

import jax
import jax.numpy as jnp
import numpy as np
from jax import lax
from jax.experimental import pallas as pl
from jax.experimental.pallas import tpu as pltpu
from jax.sharding import PartitionSpec as P

norm_eps = 1e-06
lanes = 128
wide = 256


def transform_tables(length):
    period = 2 * length
    rows = length // lanes
    kept = rows + 1
    padded = -(-kept // 16) * 16
    coarse = np.zeros((2 * padded, rows))
    grid = 2 * np.pi * (np.outer(np.arange(kept), np.arange(rows)) % (2 * rows)) / (2 * rows)
    coarse[:kept] = np.cos(grid)
    coarse[padded : padded + kept] = -np.sin(grid)
    weight = np.full((kept, 1), 2.0)
    weight[0] = weight[-1] = 1.0
    back = np.zeros((rows, 2 * padded))
    back[:, :kept] = (weight * np.cos(grid)).T / period
    back[:, padded : padded + kept] = -(weight * np.sin(grid)).T / period
    turn = 2 * np.pi * np.outer(np.arange(padded), np.arange(lanes)) / period
    fine = 2 * np.pi * (np.outer(np.arange(lanes), np.arange(lanes)) % lanes) / lanes
    cos, sin = np.cos(fine), np.sin(fine)
    forward = np.block([[cos, -sin], [sin, cos]])
    inverse = np.block([[cos, sin], [-sin, cos]])
    half = jnp.bfloat16
    return (
        coarse.astype(half),
        np.cos(turn).astype(np.float32),
        np.sin(turn).astype(np.float32),
        forward.astype(half),
        inverse.astype(half),
        back.astype(half),
    )


def mul(left, right):
    return jnp.dot(left, right, preferred_element_type=jnp.float32)


def project_kernel(tok_ref, tab_ref, taps_ref, q_ref, p_ref):
    half = jnp.bfloat16
    full = jnp.float32
    blocks, chans, _ = q_ref.shape
    vocab = tab_ref.shape[1]
    rows3 = 3 * chans
    words = lax.broadcasted_iota(jnp.int32, (vocab, wide), 0)
    lane = lax.broadcasted_iota(jnp.int32, (rows3, lanes), 1)

    def project(step, carry):
        one_back, two_back = carry
        picked = jnp.where(words == tok_ref[pl.ds(step, 1), :], 1.0, 0.0).astype(half)
        both = mul(tab_ref[...], picked).astype(half).astype(full)
        for part in range(wide // lanes):
            now = both[:, part * lanes : (part + 1) * lanes]
            once = pltpu.roll(now, 1, 1)
            twice = pltpu.roll(now, 2, 1)
            short = (
                taps_ref[0] * now
                + taps_ref[1] * jnp.where(lane < 1, one_back, once)
                + taps_ref[2] * jnp.where(lane < 2, two_back, twice)
            ).astype(half)
            one_back, two_back = once, twice
            key = short[chans : 2 * chans].astype(full)
            value = short[2 * chans :].astype(full)
            at = step * (wide // lanes) + part
            q_ref[at] = short[:chans]
            p_ref[at] = (key * value).astype(half)
        return one_back, two_back

    zero = jnp.zeros((rows3, lanes), full)
    lax.fori_loop(0, blocks * lanes // wide, project, (zero, zero))


def conv_kernel(
    q_ref, p_ref, h_ref, skip_ref,
    coarse_ref, cos_ref, sin_ref, fwd_ref, inv_ref, back_ref,
    got_ref, pf, hf, ready, send_x, recv_x, send_y, recv_y, keep,
    *, stride, unroll, chunks, groups, parts,
):
    half = jnp.bfloat16
    full = jnp.float32
    sources, chans, span = h_ref.shape
    per = span // lanes
    blocks = sources * per
    padded = cos_ref.shape[0]
    some = chans // chunks
    me = lax.axis_index("ctx")
    row = lax.axis_index("tp")
    mesh_ids = pl.DeviceIdType.MESH

    barrier = pltpu.get_barrier_semaphore()

    def greet(step, _):
        peer = lax.rem(me + step, groups)
        pl.semaphore_signal(barrier, inc=1, device_id=(peer, row), device_id_type=mesh_ids)
        return 0

    lax.fori_loop(1, groups, greet, 0)
    for step in range(1, parts):
        peer = lax.rem(row + step, parts)
        pl.semaphore_signal(barrier, inc=1, device_id=(me, peer), device_id_type=mesh_ids)

    def take(source, _):
        for part in range(per):
            tile = h_ref[source, :, part * lanes : (part + 1) * lanes]
            at = source * per + part
            hf[pl.ds(at, chans, stride=stride), :] = tile.astype(full)
            pf[pl.ds(at, chans, stride=stride), :] = p_ref[at].astype(full)
        return 0

    lax.fori_loop(0, sources, take, 0)

    def convolve(step, _):
        for sub in range(unroll):
            first = pl.multiple_of((step * unroll + sub) * stride, 8)
            here = pl.ds(first, blocks)
            pair = jnp.concatenate([pf[here, :].astype(half), hf[here, :].astype(half)], axis=1)
            staged = mul(coarse_ref[...], pair)
            cos, sin = cos_ref[...], sin_ref[...]

            def turned(lo):
                real = staged[:padded, lo : lo + lanes]
                imag = staged[padded:, lo : lo + lanes]
                return jnp.concatenate(
                    [(real * cos + imag * sin).astype(half), (imag * cos - real * sin).astype(half)],
                    axis=1,
                )

            spectra = mul(jnp.concatenate([turned(0), turned(lanes)], axis=0), fwd_ref[...])
            pr, pi = spectra[:padded, :lanes], spectra[:padded, lanes:]
            hr, hi = spectra[padded:, :lanes], spectra[padded:, lanes:]
            joint = jnp.concatenate(
                [(pr * hr - pi * hi).astype(half), (pr * hi + pi * hr).astype(half)], axis=1
            )
            undone = mul(joint, inv_ref[...])
            br, bi = undone[:, :lanes], undone[:, lanes:]
            stacked = jnp.concatenate(
                [(br * cos - bi * sin).astype(half), (bi * cos + br * sin).astype(half)], axis=0
            )
            pf[here, :] = mul(back_ref[...], stacked)
        return 0

    def across(chunk, step):
        peer = lax.rem(me + step, groups)
        return pltpu.make_async_remote_copy(
            src_ref=ready.at[chunk, peer],
            dst_ref=got_ref.at[row, me, chunk],
            send_sem=send_x.at[chunk, step],
            recv_sem=recv_x.at[chunk, step],
            device_id=(peer, row),
            device_id_type=mesh_ids,
        )

    def arrival(chunk, step):
        origin = lax.rem(me - step + groups, groups)
        slot = got_ref.at[row, origin, chunk]
        return pltpu.make_async_remote_copy(
            src_ref=slot,
            dst_ref=slot,
            send_sem=send_x.at[chunk, step],
            recv_sem=recv_x.at[chunk, step],
            device_id=(lax.rem(me + step, groups), row),
            device_id_type=mesh_ids,
        )

    def onward(chunk, step, hop, source, slot):
        return pltpu.make_async_remote_copy(
            src_ref=source,
            dst_ref=slot,
            send_sem=send_y.at[hop, chunk, step],
            recv_sem=recv_y.at[hop, chunk, step],
            device_id=(me, lax.rem(row + hop, parts)),
            device_id_type=mesh_ids,
        )

    def forward(chunk):
        def relay(step, _):
            arrival(chunk, step).wait_recv()
            slot = got_ref.at[row, lax.rem(me - step + groups, groups), chunk]
            for hop in range(1, parts):
                onward(chunk, step, hop, slot, slot).start()
            return 0

        lax.fori_loop(1, groups, relay, 0)

    for chunk in range(chunks):
        low = chunk * some
        lax.fori_loop(low // unroll, (low + some) // unroll, convolve, 0)

        def finish(source, _):
            for part in range(per):
                at = source * per + part
                convolved = pf[pl.ds(low * stride + at, some, stride=stride), :]
                product = p_ref[at, low : low + some, :].astype(full)
                skipped = (convolved + skip_ref[low : low + some, :] * product).astype(half)
                gated = q_ref[at, low : low + some, :].astype(full) * skipped.astype(full)
                ready[chunk, source, :, part * lanes : (part + 1) * lanes] = gated.astype(half)
            return 0

        lax.fori_loop(0, sources, finish, 0)
        if chunk == 0:
            pl.semaphore_wait(barrier, groups - 1 + parts - 1)

        def launch(step, _):
            across(chunk, step).start()
            return 0

        lax.fori_loop(1, groups, launch, 0)
        own = got_ref.at[row, me, chunk]
        pltpu.make_async_copy(ready.at[chunk, me], own, keep.at[chunk]).start()
        for hop in range(1, parts):
            onward(chunk, 0, hop, ready.at[chunk, me], own).start()
        if chunk > 0:
            forward(chunk - 1)
    forward(chunks - 1)

    for chunk in range(chunks):
        own = got_ref.at[row, me, chunk]
        pltpu.make_async_copy(ready.at[chunk, me], own, keep.at[chunk]).wait()

        def settle(step, _):
            across(chunk, step).wait_send()
            return 0

        lax.fori_loop(1, groups, settle, 0)

        def settle_y(step, _):
            origin = lax.rem(me - step + groups, groups)
            for hop in range(1, parts):
                mine = got_ref.at[row, origin, chunk]
                theirs = got_ref.at[lax.rem(row - hop + parts, parts), origin, chunk]
                onward(chunk, step, hop, mine, mine).wait_send()
                onward(chunk, step, hop, theirs, theirs).wait_recv()
            return 0

        lax.fori_loop(0, groups, settle_y, 0)


def project_all(tokens, table, taps, chans):
    length = tokens.shape[0]
    vmem = pl.BlockSpec(memory_space=pltpu.VMEM)
    shape = jax.ShapeDtypeStruct((length // lanes, chans, lanes), jnp.bfloat16)
    return pl.pallas_call(
        project_kernel,
        out_shape=(shape, shape),
        in_specs=[vmem] * 3,
        out_specs=(vmem, vmem),
        compiler_params=pltpu.CompilerParams(vmem_limit_bytes=24 * 1024 * 1024),
        cost_estimate=pl.CostEstimate(
            flops=2 * table.shape[0] * table.shape[1] * length * 4,
            bytes_accessed=8_000_000,
            transcendentals=0,
        ),
    )(tokens.reshape(length // wide, wide), table, taps)


def long_block(query, product, filters, skip, groups, parts):
    _, chans, span = filters.shape
    length = groups * span
    blocks = length // lanes
    stride = blocks + 8
    tables = transform_tables(length)
    chunks = 2 if chans % 32 == 0 else 1
    some = chans // chunks
    unroll = math.gcd(some, 4)
    vmem = pl.BlockSpec(memory_space=pltpu.VMEM)
    dma = pltpu.SemaphoreType.DMA
    return pl.pallas_call(
        functools.partial(
            conv_kernel,
            stride=stride, unroll=unroll, chunks=chunks, groups=groups, parts=parts,
        ),
        out_shape=jax.ShapeDtypeStruct((parts, groups, chunks, some, span), jnp.bfloat16),
        in_specs=[vmem] * 10,
        out_specs=pl.BlockSpec(memory_space=pl.ANY),
        scratch_shapes=[
            pltpu.VMEM((chans * stride, lanes), jnp.float32),
            pltpu.VMEM((chans * stride, lanes), jnp.float32),
            pltpu.VMEM((chunks, groups, some, span), jnp.bfloat16),
            dma((chunks, groups)),
            dma((chunks, groups)),
            dma((parts, chunks, groups)),
            dma((parts, chunks, groups)),
            dma((chunks,)),
        ],
        compiler_params=pltpu.CompilerParams(
            vmem_limit_bytes=48 * 1024 * 1024, collective_id=0, has_side_effects=True
        ),
        cost_estimate=pl.CostEstimate(
            flops=40_000_000_000, bytes_accessed=8_000_000, transcendentals=0
        ),
    )(query, product, filters, skip, *map(jnp.asarray, tables))


def local(token_ids, embed_table, norm_gain, w_in, short_taps, long_filter, skip_gain, w_out):
    half = jnp.bfloat16
    vocab, width = embed_table.shape
    local_channels = w_in.shape[2]
    groups = lax.axis_size("ctx")
    parts = lax.axis_size("tp")
    me = lax.axis_index("tp")
    chans = local_channels // groups
    first = lax.axis_index("ctx") * chans
    span = token_ids.shape[0]

    tokens = lax.all_gather(token_ids, "ctx", axis=0, tiled=True)
    tokens, waiting = lax.optimization_barrier((tokens, long_filter))
    filters = lax.all_to_all(
        waiting.reshape(groups, chans, span), "ctx", split_axis=0, concat_axis=0, tiled=True
    )

    rows = embed_table.astype(jnp.float32)
    scale = lax.rsqrt(jnp.mean(rows * rows, axis=1, keepdims=True) + norm_eps)
    normed = (rows * scale * norm_gain).astype(half)
    own_w = lax.dynamic_slice_in_dim(w_in, first, chans, 2).reshape(width, 3 * chans)
    table = lax.dot_general(
        own_w, normed, (((0,), (1,)), ((), ())), preferred_element_type=jnp.float32
    ).astype(half)
    taps = lax.dynamic_slice_in_dim(short_taps, first, chans, 2).reshape(-1, 3 * chans, 1)
    skip = lax.dynamic_slice_in_dim(skip_gain, first, chans)[:, None]

    query, product = project_all(tokens, table, taps, chans)
    gated = long_block(query, product, filters, skip, groups, parts)
    gated = gated.reshape(parts * local_channels, span)

    columns = w_out.shape[1]
    one_hot = (token_ids[:, None] == jnp.arange(vocab, dtype=jnp.int32)[None, :]).astype(half)
    own_embed = lax.dynamic_slice_in_dim(embed_table, me * columns, columns, 1)
    residual = jnp.dot(one_hot, own_embed, preferred_element_type=jnp.float32)
    total = lax.dot_general(
        gated, w_out, (((0,), (0,)), ((), ())), preferred_element_type=jnp.float32
    )
    return (residual + total).astype(half)


def solution(mesh):
    return jax.shard_map(
        local,
        mesh=mesh,
        in_specs=(
            P("ctx"),
            P(),
            P(),
            P(None, None, "tp"),
            P(None, None, "tp"),
            P("tp", "ctx"),
            P("tp"),
            P(None, "tp"),
        ),
        out_specs=P("ctx", "tp"),
        check_vma=False,
    )
```
